32 devices in a mesh: ga: 2 (over x), ta: 4 (over y, core), gy: 4 (over z).
Axes of the slice: x: 2, y: 2, z: 4, core: 2. Of those that a mesh axis runs over, the one named last changes fastest.
Arguments:
- clip: bfloat16 [32, 16, 64, 512], P(('ga', 'ta'), 'gy'), parts along dimension 0, may hold values from -6 to 6
- w_space: bfloat16 [3, 3, 512, 512], replicated, may hold values from -0.09375 to 0.09375
- w_time: bfloat16 [3, 512, 512], replicated, may hold values from -0.15625 to 0.15625
- w_qkv: bfloat16 [512, 1536], replicated, may hold values from -0.61871843 to 0.61871843
- w_out: bfloat16 [512, 512], replicated, may hold values from -0.25 to 0.25
- norm_gain: float32 [512], replicated, may hold values from 0.1 to 1.9
Outputs:
- block_out: bfloat16 [32, 16, 64, 512], P(('ga', 'ta'), 'gy'), parts along dimension 0
The draws below stay inside these ranges and needn't reach their ends.
There are 2 independent parts, one for each index of `ga`. The reference program is written for one: setup_inputs(seed, part) draws one part's arguments, and reference() takes and returns one part's arrays. A program takes and returns all parts, laid end to end along the dimension named above; an argument that names none is the same for every part. Nothing has to cross between parts.
All inputs are finite; a program needn't handle non-finite values.
Results may differ from the reference program's by a relative error of at most 0.0085.
Values may be sent and summed in bfloat16 or wider, within the bound.
No kernel may reach another device: no remote copies, remote signals or barrier semaphores. Data moves between devices by JAX's collectives and lax.ppermute only.
A program may use at most 64 MiB of HBM per device.

```python
import jax
import jax.numpy as jnp
from jax import lax

C = 512
HEADS = 8
WIDTH_CELLS = 64
FRAMES = 16
ROWS = 16


def draw_clip(key, part):
    full_shape = (FRAMES, ROWS, WIDTH_CELLS, C)
    normal_draw = jax.random.truncated_normal(jax.random.fold_in(key, 11), -6.0, 6.0, full_shape, jnp.float32)
    return normal_draw.astype(jnp.bfloat16)


def draw_w_qkv(key, part):
    head_width = C // HEADS
    full_shape = (C, 3, HEADS, head_width)
    weights = jax.random.truncated_normal(jax.random.fold_in(key, 23), -6.0, 6.0, full_shape, jnp.float32) * C ** (-0.5)
    return weights.reshape(C, 3 * C).astype(jnp.bfloat16)


def bell_draw(key, shape, scale, reach, kind=jnp.bfloat16):
    entries = scale * jax.random.normal(key, shape, jnp.float32)
    return jnp.clip(entries, min=-reach, max=reach).astype(kind)


def setup_inputs(seed: int = 0, part: int = 0) -> dict:
    seeds = jax.random.split(jax.random.key(seed), 7)
    part_keys = jax.random.split(jax.random.fold_in(seeds[6], part), 7)
    clip = draw_clip(jax.random.fold_in(jax.random.fold_in(seeds[6], part), 71), part)
    w_space = bell_draw(seeds[1], (3, 3, C, C), (9 * C) ** -0.5, 0.09375)
    w_time = bell_draw(seeds[2], (3, C, C), (3 * C) ** -0.5, 0.15625)
    w_qkv = draw_w_qkv(jax.random.fold_in(seeds[6], 71), part)
    w_out = bell_draw(seeds[4], (C, C), C ** -0.5, 0.25)
    norm_gain = jnp.clip(1.0 + 0.18 * jax.random.normal(seeds[5], (C,), jnp.float32), 0.1, 1.9)
    return {"clip": clip, "w_space": w_space, "w_time": w_time, "w_qkv": w_qkv, "w_out": w_out, "norm_gain": norm_gain}


def conv_space(padded, w_space, height, width):
    channels = padded.shape[-1]
    total = jnp.zeros(padded.shape[:1] + (height, width, channels), jnp.float32)
    for row_off in range(3):
        for col_off in range(3):
            window = padded[:, row_off:row_off + height, col_off:col_off + width, :]
            product = jnp.dot(window.reshape(-1, channels), w_space[row_off, col_off], preferred_element_type=jnp.float32)
            total = total + product.reshape(total.shape)
    return total

def temporal_mix(clip, hidden, earlier, w_time, norm_gain):
    channels = clip.shape[-1]
    frames = hidden.shape[0]
    joined = jnp.concatenate([earlier, hidden], axis=0)
    total = jnp.zeros(hidden.shape, jnp.float32)
    for tap_index in range(3):
        window = joined[2 - tap_index:2 - tap_index + frames]
        product = jnp.dot(window.reshape(-1, channels), w_time[tap_index], preferred_element_type=jnp.float32)
        total = total + product.reshape(hidden.shape)
    mixed = (clip.astype(jnp.float32) + total).astype(jnp.bfloat16)
    wide = mixed.astype(jnp.float32)
    scale = lax.rsqrt(lax.optimization_barrier(jnp.mean(wide * wide, axis=-1, keepdims=True)) + 1e-06)
    normed = (wide * scale * norm_gain).astype(jnp.bfloat16)
    return (mixed, normed)

def project(normed, w_qkv):
    channels = normed.shape[-1]
    flattened = jnp.dot(normed.reshape(-1, channels), w_qkv, preferred_element_type=jnp.float32).astype(jnp.bfloat16)
    joined = flattened.reshape(normed.shape[:-1] + (3 * channels,))
    return (joined[..., :channels], joined[..., channels:2 * channels], joined[..., 2 * channels:])

def attend(queries, keyset, valueset, heads):
    frames, rows, cols, channels = queries.shape
    head_dim = channels // heads
    shape = (frames, rows, cols, heads, head_dim)
    query_f = queries.reshape(shape).astype(jnp.float32)
    key_f = keyset.reshape(shape).astype(jnp.float32)
    value_f = valueset.reshape(shape).astype(jnp.float32)
    scores = jnp.einsum('frwhd,grwhd->rwhfg', query_f, key_f) * (1.0 / head_dim ** 0.5)
    peak = lax.optimization_barrier(jnp.max(scores, axis=-1, keepdims=True))
    expo = jnp.exp(scores - peak)
    probs = (expo / lax.optimization_barrier(jnp.sum(expo, axis=-1, keepdims=True))).astype(jnp.bfloat16)
    output = jnp.einsum('rwhfg,grwhd->frwhd', probs.astype(jnp.float32), value_f)
    return output.reshape(queries.shape).astype(jnp.bfloat16)

def reference(clip, w_space, w_time, w_qkv, w_out, norm_gain):
    frames, height, width, channels = clip.shape
    padded = jnp.pad(clip, ((0, 0), (1, 1), (1, 1), (0, 0)))
    hidden = jax.nn.silu(conv_space(padded, w_space, height, width)).astype(jnp.bfloat16)
    earlier = jnp.zeros((2,) + hidden.shape[1:], jnp.bfloat16)
    mixed, normed = temporal_mix(clip, hidden, earlier, w_time, norm_gain)
    queries, keyset, valueset = project(normed, w_qkv)

    def one_row(triple):
        return attend(triple[0], triple[1], triple[2], HEADS)
    stacked = tuple((jnp.moveaxis(item, 1, 0)[:, :, None] for item in (queries, keyset, valueset)))
    attended = lax.map(one_row, stacked)
    attended = jnp.moveaxis(attended[:, :, 0], 0, 1)
    projected = jnp.dot(attended.reshape(-1, channels), w_out, preferred_element_type=jnp.float32).reshape(clip.shape)
    return (mixed.astype(jnp.float32) + projected).astype(jnp.bfloat16)
```

```python
import functools

import jax
import jax.numpy as jnp
from jax import lax
from jax.experimental import pallas as pl
from jax.experimental.pallas import tpu as pltpu
from jax.sharding import PartitionSpec as P

HEADS = 8
LANE_TILE = 256
F32 = jnp.float32
BF16 = jnp.bfloat16


def padded_2(block, sides, width):
    for axis, dim in sides:
        count = lax.axis_size(axis)
        forward = [(i, i + 1) for i in range(count - 1)]
        backward = [(target, source) for source, target in forward]
        low = lax.ppermute(
            lax.slice_in_dim(block, block.shape[dim] - width, None, axis=dim), axis, forward
        )
        high = lax.ppermute(lax.slice_in_dim(block, 0, width, axis=dim), axis, backward)
        block = jnp.concatenate([low, block, high], axis=dim)
    return block


def from_behind(array, axis, by):
    devices = lax.axis_size(axis)
    pairs = [(i, i + by) for i in range(devices) if 0 <= i + by < devices]
    return lax.ppermute(array, axis, pairs)


def conv_space(padded, w_space, height, width):
    channels = padded.shape[-1]
    total = jnp.zeros(padded.shape[:1] + (height, width, channels), F32)
    for row_off in range(3):
        for col_off in range(3):
            window = padded[:, row_off : row_off + height, col_off : col_off + width, :]
            product = jnp.dot(
                window.reshape(-1, channels),
                w_space[row_off, col_off],
                preferred_element_type=F32,
            )
            total = total + product.reshape(total.shape)
    return total


def temporal_mix(clip, hidden, earlier, w_time, norm_gain):
    channels = clip.shape[-1]
    frames = hidden.shape[0]
    joined = jnp.concatenate([earlier, hidden], axis=0)
    total = jnp.zeros(hidden.shape, F32)
    for tap_index in range(3):
        window = joined[2 - tap_index : 2 - tap_index + frames]
        product = jnp.dot(
            window.reshape(-1, channels), w_time[tap_index], preferred_element_type=F32
        )
        total = total + product.reshape(hidden.shape)
    mixed = (clip.astype(F32) + total).astype(BF16)
    wide = mixed.astype(F32)
    scale = lax.rsqrt(jnp.mean(wide * wide, axis=-1, keepdims=True) + 1e-06)
    normed = (wide * scale * norm_gain).astype(BF16)
    return (mixed, normed)


def project(normed, w_qkv):
    channels = normed.shape[-1]
    flattened = jnp.dot(
        normed.reshape(-1, channels), w_qkv, preferred_element_type=F32
    ).astype(BF16)
    joined = flattened.reshape(normed.shape[:-1] + (3 * channels,))
    return (
        joined[..., :channels],
        joined[..., channels : 2 * channels],
        joined[..., 2 * channels :],
    )


def attend(queries, keyset, valueset, heads):
    frames, rows, cols, channels = queries.shape
    head_dim = channels // heads
    shape = (frames, rows, cols, heads, head_dim)
    scores = jnp.einsum(
        "frwhd,grwhd->rwhfg",
        queries.reshape(shape),
        keyset.reshape(shape),
        preferred_element_type=F32,
    )
    scores = scores * (1.0 / head_dim**0.5)
    peak = jnp.max(scores, axis=-1, keepdims=True)
    expo = jnp.exp(scores - peak)
    probs = (expo / jnp.sum(expo, axis=-1, keepdims=True)).astype(BF16)
    output = jnp.einsum(
        "rwhfg,grwhd->frwhd", probs, valueset.reshape(shape), preferred_element_type=F32
    )
    return output.reshape(queries.shape).astype(BF16)


def plain_device(clip, w_space, w_time, w_qkv, w_out, norm_gain):
    frames, height, width, channels = clip.shape
    rimmed = padded_2(clip, (("gy", 1),), 1)
    padded = jnp.pad(rimmed, ((0, 0), (0, 0), (1, 1), (0, 0)))
    hidden = jax.nn.silu(conv_space(padded, w_space, height, width)).astype(BF16)
    earlier = from_behind(hidden[-2:], "ta", 1)
    mixed, normed = temporal_mix(clip, hidden, earlier, w_time, norm_gain)
    queries, keyset, valueset = project(
        lax.all_to_all(normed, "ta", split_axis=2, concat_axis=0, tiled=True), w_qkv
    )
    output = attend(queries, keyset, valueset, HEADS)
    attended = lax.all_to_all(output, "ta", split_axis=0, concat_axis=2, tiled=True)
    projected = jnp.dot(
        attended.reshape(-1, channels), w_out, preferred_element_type=F32
    ).reshape(clip.shape)
    return (mixed.astype(F32) + projected).astype(BF16)


def pack_kernel(n, me_ref, clip_ref, *outs):
    frames, height, width, channels = clip_ref.shape
    cw = width // n
    edge, mid = outs[:n], outs[n:]
    me = me_ref[0]
    iota = lax.broadcasted_iota(jnp.int32, (2 * frames, channels), 0)
    order = [0, height - 1] + list(range(1, height - 1))
    for m in range(n):
        g = me ^ m
        here = pl.multiple_of(g * cw, cw)
        before = pl.multiple_of(jnp.maximum(g - 1, 0) * cw, cw)
        after = pl.multiple_of(jnp.minimum(g + 1, n - 1) * cw, cw)
        has_left = g > 0
        has_right = g < n - 1
        for slot, r in enumerate(order):
            dst = edge[m] if slot < 2 else mid[m]
            at = slot if slot < 2 else slot - 2
            rim = jnp.zeros((2 * frames, channels), F32)
            for f in range(frames):
                dst[at, f * cw : (f + 1) * cw, :] = clip_ref[f, r, pl.ds(here, cw), :]
                left = clip_ref[f, r, pl.ds(before, cw), :].astype(F32)[cw - 1 : cw, :]
                right = clip_ref[f, r, pl.ds(after, cw), :].astype(F32)[0:1, :]
                rim = jnp.where((iota == f) & has_left, left, rim)
                rim = jnp.where((iota == frames + f) & has_right, right, rim)
            dst[at, frames * cw : frames * (cw + 2), :] = rim.astype(BF16)


def pack(clip, me, n):
    frames, height, width, channels = clip.shape
    cw = width // n
    piece = frames * (cw + 2)
    shapes = [jax.ShapeDtypeStruct((2, piece, channels), BF16)] * n
    shapes += [jax.ShapeDtypeStruct((height - 2, piece, channels), BF16)] * n
    vm = pl.BlockSpec(memory_space=pltpu.VMEM)
    outs = pl.pallas_call(
        functools.partial(pack_kernel, n),
        out_shape=shapes,
        in_specs=[pl.BlockSpec(memory_space=pltpu.SMEM), vm],
        out_specs=[vm] * (2 * n),
        name="pack",
        compiler_params=pltpu.CompilerParams(vmem_limit_bytes=12 * 2**20),
        cost_estimate=pl.CostEstimate(flops=10**7, bytes_accessed=3 * clip.size * 2, transcendentals=0),
    )(me, clip)
    return outs[:n], outs[n:]


def main_kernel(n, frames, plan, n_edge, n_mid, has_z, *refs):
    refs = list(refs)
    me_ref = refs.pop(0)
    edge = [refs.pop(0) for _ in range(n)]
    mid = [refs.pop(0) for _ in range(n)]
    zs = [refs.pop(0) for _ in range(2)] if has_z else []
    ws_ref, wt_ref, wqkv_ref, wo_ref, gain_ref = [refs.pop(0) for _ in range(5)]
    outs = [refs.pop(0) for _ in range(n)]
    xs, hs, hb, tt, nb, mx, qkv, at, of, bias, ones = refs
    channels = gain_ref.shape[-1]
    total = n * frames
    cw = xs.shape[3]
    halves = cw // 8
    rows = len(plan)
    block = total * 8
    tokens = rows * halves * block
    nt = channels // LANE_TILE
    me = me_ref[0]

    iota = lax.broadcasted_iota(jnp.int32, (cw, channels), 0)
    for slot, (kind, index) in enumerate(sum(plan, ())):
        for m in range(n):
            base = (me ^ m) * frames
            if kind == "z":
                src = zs[index].at[m]
            else:
                src = (edge if kind == "e" else mid)[m].at[index]
            rim = src[frames * cw : frames * (cw + 2), :].astype(F32)
            for f in range(frames):
                here = src[f * cw : (f + 1) * cw, :]
                wide = here.astype(F32)
                left = jnp.where(iota == 0, rim[f : f + 1, :], pltpu.roll(wide, 1, 0))
                right = jnp.where(
                    iota == cw - 1, rim[frames + f : frames + f + 1, :], pltpu.roll(wide, cw - 1, 0)
                )
                xs[slot, 0, base + f] = left.astype(BF16)
                xs[slot, 1, base + f] = here
                xs[slot, 2, base + f] = right.astype(BF16)

    for i in range(rows):
        for ch in range(halves):
            hs[i, ch, 0:2] = jnp.zeros((2, 8, channels), F32)

    def conv_step(t, carry):
        i, j = t // nt, t % nt
        cols = pl.ds(pl.multiple_of(j * LANE_TILE, LANE_TILE), LANE_TILE)
        acc = jnp.zeros((total * cw, LANE_TILE), F32)
        for a in range(3):
            for b in range(3):
                lhs = xs[3 * i + a, b].reshape(total * cw, channels)
                acc = acc + jnp.dot(lhs, ws_ref[a, b, :, cols], preferred_element_type=F32)
        hidden = (acc * jax.nn.sigmoid(acc)).reshape(total, halves, 8, LANE_TILE)
        for ch in range(halves):
            hs[i, ch, 2:, :, cols] = hidden[:, ch]
        return carry

    lax.fori_loop(0, rows * nt, conv_step, 0)

    for k in range(3):
        for i in range(rows):
            for ch in range(halves):
                first = (i * halves + ch) * block
                hb[k, first : first + block, :] = (
                    hs[i, ch, 2 - k : 2 - k + total].reshape(block, channels).astype(BF16)
                )
    per_row = halves * block

    def time_step(t, carry):
        i, j = t // nt, t % nt
        cols = pl.ds(pl.multiple_of(j * LANE_TILE, LANE_TILE), LANE_TILE)
        span = pl.ds(pl.multiple_of(i * per_row, per_row), per_row)
        acc = jnp.zeros((per_row, LANE_TILE), F32)
        for k in range(3):
            acc = acc + jnp.dot(hb[k, span, :], wt_ref[k, :, cols], preferred_element_type=F32)
        tt[span, cols] = acc
        return carry

    lax.fori_loop(0, rows * nt, time_step, 0)

    gain = gain_ref[...]

    def norm_step(i, carry):
        clip = xs[3 * i + 1, 1].astype(F32).reshape(total, halves, 8, channels)
        for ch in range(halves):
            span = pl.ds(pl.multiple_of((i * halves + ch) * block, block), block)
            mixed = (clip[:, ch].reshape(block, channels) + tt[span, :]).astype(BF16)
            wide = mixed.astype(F32)
            scale = lax.rsqrt(jnp.mean(wide * wide, axis=-1, keepdims=True) + 1e-06)
            mx[span, :] = mixed
            nb[span, :] = (wide * scale * gain).astype(BF16)
        return carry

    lax.fori_loop(0, rows, norm_step, 0)

    head_dim = channels // HEADS
    root = 1.0 / head_dim**0.5

    def qkv_step(t, carry):
        i, j = t // (3 * nt), t % (3 * nt)
        cols = pl.ds(pl.multiple_of(j * LANE_TILE, LANE_TILE), LANE_TILE)
        span = pl.ds(pl.multiple_of(i * per_row, per_row), per_row)
        product = jnp.dot(nb[span, :], wqkv_ref[:, cols], preferred_element_type=F32)
        qkv[span, cols] = product.astype(BF16)
        return carry

    lax.fori_loop(0, rows * 3 * nt, qkv_step, 0)

    pair = 2 * head_dim
    ri = lax.broadcasted_iota(jnp.int32, (block, 2 * block), 0) % 8
    ci = lax.broadcasted_iota(jnp.int32, (block, 2 * block), 1) % 8
    bias[...] = jnp.where(ri == ci, 0.0, -1e30).astype(F32)
    oi = lax.broadcasted_iota(jnp.int32, (2 * block, pair), 0) // block
    ol = lax.broadcasted_iota(jnp.int32, (2 * block, pair), 1) // head_dim
    ones[...] = jnp.where(oi == ol, 1.0, 0.0).astype(BF16)

    def attend_step(b, carry):
        span = pl.ds(pl.multiple_of(b * block, block), block)
        low = lax.broadcasted_iota(jnp.int32, (block, pair), 1) < head_dim
        zero = jnp.zeros((block, pair), BF16)
        for p in range(channels // pair):
            q = qkv[span, p * pair : (p + 1) * pair] * jnp.asarray(root, BF16)
            k = qkv[span, channels + p * pair : channels + (p + 1) * pair]
            v = qkv[span, 2 * channels + p * pair : 2 * channels + (p + 1) * pair]
            keys = jnp.concatenate([jnp.where(low, k, zero), jnp.where(low, zero, k)], axis=0)
            vals = jnp.concatenate([jnp.where(low, v, zero), jnp.where(low, zero, v)], axis=0)
            s = lax.dot_general(q, keys, (((1,), (1,)), ((), ())), preferred_element_type=F32)
            s = s + bias[...]
            s0, s1 = s[:, :block], s[:, block:]
            e0 = jnp.exp(s0 - jnp.max(s0, axis=-1, keepdims=True)).astype(BF16)
            e1 = jnp.exp(s1 - jnp.max(s1, axis=-1, keepdims=True)).astype(BF16)
            probs = jnp.concatenate([e0, e1], axis=1)
            rhs = jnp.concatenate([vals, ones[...]], axis=1)
            o = jnp.dot(probs, rhs, preferred_element_type=F32)
            at[span, p * pair : (p + 1) * pair] = (o[:, :pair] / o[:, pair:]).astype(BF16)
        return carry

    lax.fori_loop(0, rows * halves, attend_step, 0)

    def out_step(t, carry):
        i, j = t // nt, t % nt
        cols = pl.ds(pl.multiple_of(j * LANE_TILE, LANE_TILE), LANE_TILE)
        span = pl.ds(pl.multiple_of(i * per_row, per_row), per_row)
        product = jnp.dot(at[span, :], wo_ref[:, cols], preferred_element_type=F32)
        result = (mx[span, cols].astype(F32) + product).reshape(halves, total, 8, LANE_TILE)
        of[i, :, :, :, cols] = result
        return carry

    lax.fori_loop(0, rows * nt, out_step, 0)
    for m in range(n):
        base = (me ^ m) * frames
        for i in range(rows):
            parts = [of[i, ch, pl.ds(base, frames)] for ch in range(halves)]
            outs[m][i] = jnp.concatenate(parts, axis=1).astype(BF16)


def main(me, edge, mid, zs, weights, plan, frames, cw, name):
    n = len(edge)
    w_space, w_time, w_qkv, w_out, norm_gain = weights
    channels = w_out.shape[0]
    total = n * frames
    rows = len(plan)
    halves = cw // 8
    block = total * 8
    tokens = rows * halves * block
    vm = pl.BlockSpec(memory_space=pltpu.VMEM)
    n_in = 2 * n + len(zs) + 5
    return pl.pallas_call(
        functools.partial(main_kernel, n, frames, plan, 2, mid[0].shape[0], bool(zs)),
        out_shape=[jax.ShapeDtypeStruct((rows, frames, cw, channels), BF16)] * n,
        in_specs=[pl.BlockSpec(memory_space=pltpu.SMEM)] + [vm] * n_in,
        out_specs=[vm] * n,
        scratch_shapes=[
            pltpu.VMEM((3 * rows, 3, total, cw, channels), BF16),
            pltpu.VMEM((rows, halves, total + 2, 8, channels), F32),
            pltpu.VMEM((3, tokens, channels), BF16),
            pltpu.VMEM((tokens, channels), F32),
            pltpu.VMEM((tokens, channels), BF16),
            pltpu.VMEM((tokens, channels), BF16),
            pltpu.VMEM((tokens, 3 * channels), BF16),
            pltpu.VMEM((tokens, channels), BF16),
            pltpu.VMEM((rows, halves, total, 8, channels), F32),
            pltpu.VMEM((block, 2 * block), F32),
            pltpu.VMEM((2 * block, 2 * channels // HEADS), BF16),
        ],
        name=name,
        compiler_params=pltpu.CompilerParams(vmem_limit_bytes=32 * 2**20),
        cost_estimate=pl.CostEstimate(
            flops=2 * tokens * channels * channels * 16, bytes_accessed=10**6, transcendentals=tokens * channels
        ),
    )(me, *edge, *mid, *zs, w_space, w_time, w_qkv, w_out, norm_gain.reshape(1, channels))


def join_kernel(n, me_ref, *refs):
    outer, inner, out_ref = refs[:n], refs[n : 2 * n], refs[2 * n]
    frames, height, width, channels = out_ref.shape
    cw = width // n
    me = me_ref[0]
    order = [0, height - 1] + list(range(1, height - 1))
    for m in range(n):
        at = pl.ds(pl.multiple_of((me ^ m) * cw, cw), cw)
        for slot, r in enumerate(order):
            src = outer[m].at[slot] if slot < 2 else inner[m].at[slot - 2]
            for f in range(frames):
                out_ref[f, r, at, :] = src[f]


def join(me, outer, inner, shape):
    n = len(outer)
    vm = pl.BlockSpec(memory_space=pltpu.VMEM)
    return pl.pallas_call(
        functools.partial(join_kernel, n),
        out_shape=jax.ShapeDtypeStruct(shape, BF16),
        in_specs=[pl.BlockSpec(memory_space=pltpu.SMEM)] + [vm] * (2 * n),
        out_specs=vm,
        name="join",
        compiler_params=pltpu.CompilerParams(vmem_limit_bytes=12 * 2**20),
    )(me, *outer, *inner)


def kernel_device(clip, w_space, w_time, w_qkv, w_out, norm_gain):
    frames, height, width, channels = clip.shape
    n = lax.axis_size("ta")
    cw = width // n
    me = lax.axis_index("ta").astype(jnp.int32).reshape(1)
    weights = (w_space, w_time, w_qkv, w_out, norm_gain)

    def swap(pieces):
        return [pieces[0]] + [
            lax.ppermute(pieces[m], "ta", [(i, i ^ m) for i in range(n)]) for m in range(1, n)
        ]

    edge, mid = pack(clip, me, n)
    edge = swap(edge)
    mid = swap(mid)
    count = lax.axis_size("gy")
    forward = [(i, i + 1) for i in range(count - 1)]
    backward = [(b, a) for a, b in forward]
    above = lax.ppermute(jnp.stack([e[1] for e in edge]), "gy", forward)
    below = lax.ppermute(jnp.stack([e[0] for e in edge]), "gy", backward)

    def where(r):
        if r < 0:
            return ("z", 0)
        if r >= height:
            return ("z", 1)
        if r == 0:
            return ("e", 0)
        if r == height - 1:
            return ("e", 1)
        return ("m", r - 1)

    def plan(rows):
        return tuple(tuple(where(r + a - 1) for a in range(3)) for r in rows)

    inner = main(me, edge, mid, [], weights, plan(range(1, height - 1)), frames, cw, "inner")
    inner = swap(inner)
    outer = main(me, edge, mid, [above, below], weights, plan([0, height - 1]), frames, cw, "outer")
    outer = swap(outer)
    return join(me, outer, inner, clip.shape)


def solution(mesh):
    n = mesh.shape["ta"]
    rows_axis = mesh.shape["gy"]

    def per_device(clip, w_space, w_time, w_qkv, w_out, norm_gain):
        frames, height, width, channels = clip.shape
        tiled = (
            n & (n - 1) == 0
            and width % n == 0
            and (width // n) % 16 == 0
            and (2 * frames) % 8 == 0
            and frames * n * 8 == 128
            and height >= 3
            and channels % LANE_TILE == 0
            and 2 * channels // HEADS == 128
        )
        device = kernel_device if tiled else plain_device
        return device(clip, w_space, w_time, w_qkv, w_out, norm_gain)

    in_specs = (P(("ga", "ta"), "gy", None, None), P(), P(), P(), P(), P())
    out_specs = P(("ga", "ta"), "gy", None, None)
    return jax.shard_map(
        per_device, mesh=mesh, in_specs=in_specs, out_specs=out_specs, check_vma=False
    )
```
